32 devices in a mesh: seq: 8 (over y, x, core), kvh: 4 (over z).
Axes of the slice: x: 2, y: 2, z: 4, core: 2. Of those that a mesh axis runs over, the one named last changes fastest.
Arguments:
- queries: bfloat16 [64, 64, 128], P(None, 'kvh'), may hold values from -128 to 128
- keys: bfloat16 [1024, 8, 128, 128], P('seq', 'kvh'), may hold values from -6 to 6
- values: bfloat16 [1024, 8, 128, 128], P('seq', 'kvh'), may hold values from -6 to 6
- rep_keys: bfloat16 [1024, 8, 4, 128], P('seq', 'kvh'), may hold values from -8 to 8
- rep_values: bfloat16 [1024, 8, 4, 128], P('seq', 'kvh'), may hold values from -6 to 6
- block_ids: int32 [64, 8, 16], P(None, 'kvh'), may hold values from 0 to 1023, as said below
- block_counts: int32 [1024], P('seq'), may hold values from 64 to 128
- out_weight: bfloat16 [8192, 8192], P('kvh', 'seq'), may hold values from -0.5 to 0.5
Outputs:
- projected: bfloat16 [64, 8192], P('kvh', 'seq')
The draws below stay inside these ranges and needn't reach their ends.
Inputs may be any that keep to these rules, and one draw needn't show every extreme that they name: `block_ids`: for every token and key-value head the 16 ids are different. For every key-value head at most 192 of its 64 x 16 ids lie among the blocks o * 128 to (o + 1) * 128 - 1 of one o, and for some o exactly 192.
All inputs are finite; a program needn't handle non-finite values.
Results may differ from the reference program's by a relative error of at most 0.023.
Values may be sent and summed in bfloat16 or wider, within the bound.
A program may use at most 128 MiB of HBM per device.

```python
import math
import jax
import jax.numpy as jnp
from jax import lax

DM = 8192
H = 64
KVH = 8
HD = 128
BS = 128
R = 4
TOPK = 16
B = 64
BLK_DEV = 128
NB = 1024


def summary_base(key):
    drawn = jax.random.normal(jax.random.fold_in(key, 11), (NB, KVH, R, HD), jnp.float32)
    return jnp.clip(drawn, -6.0, 6.0)


def draw_rep_keys(key, part):
    summary = summary_base(key)
    return summary.astype(jnp.bfloat16)


def draw_queries(key, part):
    query_base = jnp.clip(jax.random.normal(jax.random.fold_in(key, 12), (B, H, HD), jnp.float32), -6.0, 6.0)
    return query_base.astype(jnp.bfloat16)


def draw_block_ids(key, part):
    shards = NB // BLK_DEV
    hot_shard = jax.random.randint(jax.random.fold_in(key, 21), (1, KVH, 1), 0, shards)
    turn_shift = jax.random.randint(jax.random.fold_in(key, 22), (1, KVH, 1), 0, shards - 1)
    token_pos = jnp.arange(B, dtype=jnp.int32).reshape(B, 1, 1)
    slot_pos = jnp.arange(TOPK, dtype=jnp.int32).reshape(1, 1, TOPK)
    spread = (hot_shard + 1 + (token_pos * 13 + slot_pos + turn_shift) % (shards - 1)) % shards
    owners = jnp.where(slot_pos < 3, hot_shard, spread)
    noise = jax.random.randint(jax.random.fold_in(key, 23), (B, KVH, BLK_DEV), 0, 1 << 20)
    ranked = noise * BLK_DEV + jnp.arange(BLK_DEV, dtype=jnp.int32)
    offsets = lax.top_k(ranked, TOPK)[1].astype(jnp.int32)
    picked = owners * BLK_DEV + offsets
    shuffle = jax.random.randint(jax.random.fold_in(key, 24), (B, KVH, TOPK), 0, 1 << 20) * TOPK + jnp.arange(TOPK, dtype=jnp.int32)
    order_ids = lax.top_k(shuffle, TOPK)[1].astype(jnp.int32)
    return jnp.take_along_axis(picked, order_ids, axis=2).astype(jnp.int32)


def plant(values, stream_key, least, high):
    shape = values.shape
    place = [jax.random.randint(jax.random.fold_in(stream_key, axis), (), 0, shape[axis]) for axis in range(len(shape))]
    values = values.at[tuple(place)].set(least)
    longest = shape.index(max(shape))
    place[longest] = (place[longest] + 1) % shape[longest]
    return values.at[tuple(place)].set(high)


def levels(stream_key, extent, pieces, smallest, largest):
    level, own = 1.0, jax.random.fold_in(stream_key, 6)
    for axis_at, blocks in pieces:
        heights = jnp.exp(jax.random.uniform(jax.random.fold_in(own, axis_at), (blocks,), jnp.float32, smallest / len(pieces), largest / len(pieces)))
        level = level * jnp.repeat(heights, extent[axis_at] // blocks).reshape([-1 if axis == axis_at else 1 for axis in range(len(extent))])
    return level


def scatter_about(key, extent, scale, bound, cuts=(), kind=jnp.bfloat16):
    factor_of = levels(key, extent, cuts, -0.22, 0.18) if cuts else 1.0
    array = jax.random.normal(key, extent, jnp.float32) * scale * factor_of
    return jnp.minimum(jnp.maximum(array, -bound), bound).astype(kind)


def setup_inputs(seed: int = 0) -> dict:
    seeds = jax.random.split(jax.random.key(seed), 9)
    queries = draw_queries(jax.random.fold_in(seeds[8], 71), 0)
    keys = scatter_about(seeds[1], (NB, KVH, BS, HD), 1.0, 6.0, ((0, 8), (1, 4)))
    values = scatter_about(seeds[2], (NB, KVH, BS, HD), 1.0, 6.0, ((0, 8), (1, 4)))
    rep_keys = draw_rep_keys(jax.random.fold_in(seeds[8], 71), 0)
    rep_values = scatter_about(seeds[4], (NB, KVH, R, HD), 1.0, 6.0, ((0, 8), (1, 4)))
    block_ids = draw_block_ids(jax.random.fold_in(seeds[8], 71), 0)
    block_counts = plant(jax.random.randint(seeds[6], (NB,), BS // 2, BS + 1), jax.random.fold_in(seeds[6], 1), BS // 2, BS).astype(jnp.int32)
    out_weight = scatter_about(seeds[7], (H * HD, DM), HD ** -0.5, 0.5, ((0, 4), (1, 8)))
    return {"queries": queries, "keys": keys, "values": values, "rep_keys": rep_keys, "rep_values": rep_values, "block_ids": block_ids, "block_counts": block_counts, "out_weight": out_weight}


FLOOR_SCORE = -1e+30

def reference(queries, keys, values, rep_keys, rep_values, block_ids, block_counts, out_weight):
    group_size = H // KVH
    inv_root = 1.0 / math.sqrt(HD)

    def one_head(kv_head):
        query_rows = lax.dynamic_slice_in_dim(queries, kv_head * group_size, group_size, 1).astype(jnp.float32)
        summary_keys = jnp.take(rep_keys, kv_head, axis=1).reshape(NB * R, HD).astype(jnp.float32)
        summary_vals = jnp.take(rep_values, kv_head, axis=1).reshape(NB * R, HD).astype(jnp.float32)
        block_rows = jnp.take(block_ids, kv_head, axis=1)
        tile_keys = keys[block_rows, kv_head].astype(jnp.float32)
        tile_vals = values[block_rows, kv_head].astype(jnp.float32)
        valid_map = jnp.arange(BS, dtype=jnp.int32)[None, None, :] < block_counts[block_rows][:, :, None]
        summary_scores = jnp.einsum('bgd,nd->bgn', query_rows, summary_keys) * inv_root
        chosen_scores = jnp.einsum('bgd,bstd->bgst', query_rows, tile_keys) * inv_root
        chosen_scores = jnp.where(valid_map[:, None], chosen_scores, FLOOR_SCORE)
        highest = jnp.maximum(lax.optimization_barrier(jnp.max(summary_scores, axis=2)), lax.optimization_barrier(jnp.max(chosen_scores, axis=(2, 3))))
        summary_weights = jnp.exp(summary_scores - highest[:, :, None])
        chosen_weights = jnp.where(valid_map[:, None], jnp.exp(chosen_scores - highest[:, :, None, None]), 0.0)
        weight_sum = lax.optimization_barrier(jnp.sum(summary_weights, axis=2)) + lax.optimization_barrier(jnp.sum(chosen_weights, axis=(2, 3)))
        summary_round = lax.optimization_barrier(summary_weights.astype(jnp.bfloat16)).astype(jnp.float32)
        chosen_round = lax.optimization_barrier(chosen_weights.astype(jnp.bfloat16)).astype(jnp.float32)
        weighted = jnp.einsum('bgn,nd->bgd', summary_round, summary_vals)
        weighted = weighted + jnp.einsum('bgst,bstd->bgd', chosen_round, tile_vals)
        return (weighted / weight_sum[:, :, None]).astype(jnp.bfloat16)
    heads_out = lax.map(one_head, jnp.arange(KVH, dtype=jnp.int32))
    attended = jnp.transpose(heads_out, (1, 0, 2, 3)).reshape(B, H * HD)
    return jnp.dot(attended, out_weight, preferred_element_type=jnp.float32).astype(jnp.bfloat16)
```

```python
import functools
import math

import jax
import jax.numpy as jnp
from jax import lax
from jax.experimental import pallas as pl
from jax.experimental.pallas import tpu as pltpu
from jax.sharding import PartitionSpec as P

FLOOR_SCORE = -1e30
LANES = 128
UNROLL = 16
PIECES = 4
MESH = pl.DeviceIdType.MESH


def contract_last(a, b):
    return lax.dot_general(a, b, (((1,), (1,)), ((), ())), preferred_element_type=jnp.float32)


def matmul(a, b):
    return jnp.dot(a, b, preferred_element_type=jnp.float32)


def attend_kernel(
    counts_ref, ids_ref, q_ref, rk_ref, rv_ref, keys_ref, values_ref, o_ref, lse_ref,
    k_mem, v_mem, slots_v, slots_s, qh, sums, sc, top, low, acc, k_sem, v_sem, slot_sem,
):
    tokens, heads, width = q_ref.shape
    kv_heads, blocks, span, _ = k_mem.shape
    group = heads // kv_heads
    reps = rk_ref.shape[1]
    chosen = ids_ref.shape[2]
    lanes = slots_v.shape[1]
    inv_root = 1.0 / math.sqrt(width)
    me = lax.axis_index("seq")

    part = blocks // PIECES

    def copy_of(k, i, source, target, sem):
        rows = pl.ds(i * part, part)
        return pltpu.make_async_copy(source.at[rows, k], target.at[k, rows], sem.at[k, i])

    for k in range(kv_heads):
        for i in range(PIECES):
            copy_of(k, i, keys_ref, k_mem, k_sem).start()
        for i in range(PIECES):
            copy_of(k, i, values_ref, v_mem, v_sem).start()

    token_of = lax.broadcasted_iota(jnp.int32, (tokens, chosen), 0)
    slot_of = lax.broadcasted_iota(jnp.int32, (tokens, lanes), 1)
    before_slot = (
        lax.broadcasted_iota(jnp.int32, (chosen, chosen), 0)
        < lax.broadcasted_iota(jnp.int32, (chosen, chosen), 1)
    ).astype(jnp.bfloat16)
    before_token = (
        lax.broadcasted_iota(jnp.int32, (tokens, tokens), 1)
        < lax.broadcasted_iota(jnp.int32, (tokens, tokens), 0)
    ).astype(jnp.bfloat16)
    every_slot = jnp.ones((chosen, chosen), jnp.bfloat16)
    slots_v[...] = jnp.zeros_like(slots_v)
    for k in range(kv_heads):
        ids = ids_ref[:, k, :] - me * blocks
        here = (ids >= 0) & (ids < blocks)
        mark = jnp.where(here, 1.0, 0.0).astype(jnp.bfloat16)
        of_token = matmul(mark, every_slot)
        rank = matmul(mark, before_slot) + matmul(before_token, of_token.astype(jnp.bfloat16))
        rank = jnp.where(here, rank.astype(jnp.int32), -1)
        code = token_of * blocks + ids + 1
        found = jnp.zeros((tokens, lanes), jnp.int32)
        for s in range(chosen):
            found = found + jnp.where(rank[:, s : s + 1] == slot_of, code[:, s : s + 1], 0)
        slots_v[k : k + 1, :] = jnp.sum(found, axis=0, keepdims=True)
        total = jnp.sum(of_token[:, 0:1], axis=0, keepdims=True).astype(jnp.int32)
        slots_v[kv_heads + k : kv_heads + k + 1, :] = jnp.broadcast_to(total, (1, lanes))
    slot_copy = pltpu.make_async_copy(slots_v, slots_s, slot_sem)
    slot_copy.start()

    for k in range(kv_heads):
        mine = q_ref[...].astype(jnp.float32)[:, k * group : (k + 1) * group, :]
        qh[k] = mine.reshape(tokens * group, width).astype(jnp.bfloat16)
        scores = contract_last(qh[k], rk_ref[k]) * inv_root
        sums[k] = scores
        most = scores[:, :LANES]
        for c in range(LANES, reps, LANES):
            most = jnp.maximum(most, scores[:, c : c + LANES])
        top[k] = most.reshape(tokens, group, LANES)

    slot_copy.wait()
    lane = lax.broadcasted_iota(jnp.int32, (group, span), 1)

    def slot(k, j):
        code = slots_s[k, j]
        at = jnp.maximum(code - 1, 0)
        token = lax.div(at, blocks)
        return code, token, at - token * blocks

    for k in range(kv_heads):
        rounds = lax.div(slots_s[kv_heads + k, 0] + (UNROLL - 1), UNROLL)

        for i in range(PIECES):
            copy_of(k, i, keys_ref, k_mem, k_sem).wait()

        def score_round(i, carry, k=k):
            places, found = [], []
            for u in range(UNROLL):
                j = i * UNROLL + u
                code, token, block = slot(k, j)
                count = jnp.where(code > 0, counts_ref[block], 0)
                s = contract_last(q_ref[token], k_mem[k, block])
                s = s[k * group : (k + 1) * group] * inv_root
                s = jnp.where(lane < count, s, FLOOR_SCORE)
                sc[j] = s
                places.append(token)
                found.append(s)
            for token, s in zip(places, found):
                top[k, token] = jnp.maximum(top[k, token], s)
            return carry

        lax.fori_loop(0, rounds, score_round, 0)

        most = jnp.max(top[k], axis=2, keepdims=True)
        top[k] = jnp.broadcast_to(most, (tokens, group, LANES))
        weights = jnp.exp(sums[k] - most.reshape(tokens * group, 1))
        some = weights[:, :LANES]
        for c in range(LANES, reps, LANES):
            some = some + weights[:, c : c + LANES]
        low[k] = some.reshape(tokens, group, LANES)
        acc[k] = matmul(weights.astype(jnp.bfloat16), rv_ref[k]).reshape(tokens, group, width)

        for i in range(PIECES):
            copy_of(k, i, values_ref, v_mem, v_sem).wait()

        def weight_round(i, carry, k=k):
            places, found, parts = [], [], []
            for u in range(UNROLL):
                j = i * UNROLL + u
                _, token, block = slot(k, j)
                p = jnp.exp(sc[j] - top[k, token])
                places.append(token)
                found.append(p)
                parts.append(matmul(p.astype(jnp.bfloat16), v_mem[k, block]))
            for token, p, o in zip(places, found, parts):
                low[k, token] = low[k, token] + p
                acc[k, token] = acc[k, token] + o
            return carry

        lax.fori_loop(0, rounds, weight_round, 0)

        weight_sum = jnp.sum(low[k], axis=2, keepdims=True)
        low[k] = top[k] + jnp.log(jnp.broadcast_to(weight_sum, (tokens, group, LANES)))
        acc[k] = acc[k] / weight_sum

    shares, rows, _ = o_ref.shape
    run = min(rows, tokens)
    diagonal = lax.broadcasted_iota(jnp.int32, (run, LANES), 0)
    column = lax.broadcasted_iota(jnp.int32, (run, LANES), 1)
    for share in range(shares):
        line = jnp.zeros((1, LANES), jnp.float32)
        for at in range(0, rows, run):
            head, token = divmod(share * rows + at, tokens)
            k, g = divmod(head, group)
            o_ref[share, at : at + run, :] = acc[k, token : token + run, g, :].astype(jnp.bfloat16)
            lse = low[k, token : token + run, g, :]
            line += jnp.sum(
                jnp.where(diagonal + at == column, lse, 0.0), axis=0, keepdims=True
            )
        lse_ref[share] = jnp.broadcast_to(line, lse_ref.shape[1:])


def finish_kernel(
    shares, groups, o_ref, lse_ref, w_ref, out_ref,
    w_mem, o_in, lse_in, attended, total, part_out, part_in,
    w_sem, o_send, o_recv, lse_send, lse_recv, a_send, a_recv, p_send, p_recv,
):
    me, mine = lax.axis_index("seq"), lax.axis_index("kvh")
    _, rows, width = o_ref.shape
    tokens, columns = total.shape

    def w_copy(i):
        depth = w_ref.shape[0] // shares
        return pltpu.make_async_copy(
            w_ref.at[pl.ds(i * depth, depth)], w_mem.at[pl.ds(i * depth, depth)], w_sem.at[i]
        )

    for i in range(shares):
        w_copy(i).start()

    barrier = pltpu.get_barrier_semaphore()
    for d in range(1, shares):
        pl.semaphore_signal(
            barrier, inc=1, device_id={"seq": lax.rem(me + d, shares)}, device_id_type=MESH
        )
    for d in range(1, groups):
        pl.semaphore_signal(
            barrier, inc=1, device_id={"kvh": lax.rem(mine + d, groups)}, device_id_type=MESH
        )
    pl.semaphore_wait(barrier, shares - 1 + groups - 1)

    def send(source, target, sent, got, axis, peer):
        copy = pltpu.make_async_remote_copy(
            src_ref=source, dst_ref=target, send_sem=sent, recv_sem=got,
            device_id={axis: peer}, device_id_type=MESH,
        )
        copy.start()
        return copy

    spread = []
    for d in range(1, shares):
        peer = lax.rem(me + d, shares)
        spread.append(send(
            lse_ref.at[peer], lse_in.at[me], lse_send.at[d], lse_recv.at[d], "seq", peer))
        spread.append(send(o_ref.at[peer], o_in.at[me], o_send.at[d], o_recv.at[d], "seq", peer))
    lse_in[me] = lse_ref[me]
    o_in[me] = o_ref[me]
    for copy in spread:
        copy.wait_recv()

    lse = [lse_in[i][0:1] for i in range(shares)]
    highest = functools.reduce(jnp.maximum, lse)
    factors = [jnp.exp(one - highest) for one in lse]
    inverse = 1.0 / functools.reduce(jnp.add, factors)
    on_diagonal = lax.broadcasted_iota(jnp.int32, (rows, LANES), 0) == lax.broadcasted_iota(
        jnp.int32, (rows, LANES), 1
    )
    joined = jnp.zeros((rows, width), jnp.float32)
    for i in range(shares):
        factor = jnp.where(on_diagonal, factors[i] * inverse, 0.0)
        joined += jnp.sum(factor, axis=1, keepdims=True) * o_in[i].astype(jnp.float32)
    attended[me] = joined.astype(jnp.bfloat16)

    gathered = []
    for d in range(1, shares):
        peer = lax.rem(me + d, shares)
        gathered.append(send(
            attended.at[me], attended.at[me], a_send.at[d], a_recv.at[d], "seq", peer))

    for i in range(shares):
        w_copy(i).wait()
    if rows % tokens == 0:
        depth = rows // tokens * width
        for d in range(shares):
            if d:
                gathered[d - 1].wait_recv()
            owner = lax.rem(me - d + shares, shares)
            block = attended[owner]
            left = jnp.concatenate(
                [block[at : at + tokens] for at in range(0, rows, tokens)], axis=1
            )
            right = w_mem[pl.ds(pl.multiple_of(owner * depth, depth), depth), :]
            term = matmul(left, right)
            total[...] = term if d == 0 else total[...] + term
    else:
        for copy in gathered:
            copy.wait_recv()
        pieces = tokens // rows
        for head in range(shares // pieces):
            left = jnp.concatenate([attended[head * pieces + p] for p in range(pieces)], axis=0)
            term = matmul(left, w_mem[head * width : (head + 1) * width, :])
            total[...] = term if head == 0 else total[...] + term

    here = tokens // groups
    part_out[...] = total[...].astype(jnp.bfloat16).reshape(part_out.shape)
    parts = []
    for d in range(1, groups):
        peer = lax.rem(mine + d, groups)
        parts.append(send(
            part_out.at[peer], part_in.at[mine], p_send.at[d], p_recv.at[d], "kvh", peer))
    result = total[pl.ds(pl.multiple_of(mine * here, here), here), :]
    for d in range(1, groups):
        parts[d - 1].wait_recv()
        result = result + part_in[lax.rem(mine - d + groups, groups)].astype(jnp.float32)
    out_ref[...] = result.astype(out_ref.dtype)
    for copy in spread + gathered + parts:
        copy.wait_send()


def on_device(
    shares, groups, queries, keys, values, rep_keys, rep_values, block_ids, block_counts, out_weight
):
    tokens, heads, width = queries.shape
    blocks, kv_heads, span, _ = keys.shape
    group = heads // kv_heads
    reps = blocks * rep_keys.shape[2]
    rows = heads * tokens // shares
    columns = out_weight.shape[1]
    capacity = -(-3 * tokens // UNROLL) * UNROLL
    lanes = -(-capacity // LANES) * LANES
    vmem = pl.BlockSpec(memory_space=pltpu.VMEM)
    smem = pl.BlockSpec(memory_space=pltpu.SMEM)
    hbm = pl.BlockSpec(memory_space=pl.ANY)
    dma = pltpu.SemaphoreType.DMA

    def by_head(reps_of):
        return jnp.transpose(reps_of, (1, 0, 2, 3)).reshape(kv_heads, reps, width)

    partial, lse = pl.pallas_call(
        attend_kernel,
        out_shape=(
            jax.ShapeDtypeStruct((shares, rows, width), jnp.bfloat16),
            jax.ShapeDtypeStruct((shares, 8, LANES), jnp.float32),
        ),
        in_specs=[smem, vmem, vmem, vmem, vmem, hbm, hbm],
        out_specs=(vmem, vmem),
        scratch_shapes=[
            pltpu.VMEM((kv_heads, blocks, span, width), jnp.bfloat16),
            pltpu.VMEM((kv_heads, blocks, span, width), jnp.bfloat16),
            pltpu.VMEM((8, lanes), jnp.int32),
            pltpu.SMEM((8, lanes), jnp.int32),
            pltpu.VMEM((kv_heads, tokens * group, width), jnp.bfloat16),
            pltpu.VMEM((kv_heads, tokens * group, reps), jnp.float32),
            pltpu.VMEM((capacity, group, span), jnp.float32),
            pltpu.VMEM((kv_heads, tokens, group, LANES), jnp.float32),
            pltpu.VMEM((kv_heads, tokens, group, LANES), jnp.float32),
            pltpu.VMEM((kv_heads, tokens, group, width), jnp.float32),
            dma((kv_heads, PIECES)),
            dma((kv_heads, PIECES)),
            dma,
        ],
        compiler_params=pltpu.CompilerParams(vmem_limit_bytes=40 * 1024 * 1024),
    )(block_counts, block_ids, queries, by_head(rep_keys), by_head(rep_values), keys, values)

    return pl.pallas_call(
        functools.partial(finish_kernel, shares, groups),
        out_shape=jax.ShapeDtypeStruct((tokens // groups, columns), jnp.bfloat16),
        in_specs=[vmem, vmem, hbm],
        out_specs=vmem,
        scratch_shapes=[
            pltpu.VMEM(out_weight.shape, jnp.bfloat16),
            pltpu.VMEM((shares, rows, width), jnp.bfloat16),
            pltpu.VMEM((shares, 8, LANES), jnp.float32),
            pltpu.VMEM((shares, rows, width), jnp.bfloat16),
            pltpu.VMEM((tokens, columns), jnp.float32),
            pltpu.VMEM((groups, tokens // groups, columns), jnp.bfloat16),
            pltpu.VMEM((groups, tokens // groups, columns), jnp.bfloat16),
            dma((shares,)),
            dma((shares,)),
            dma((shares,)),
            dma((shares,)),
            dma((shares,)),
            dma((shares,)),
            dma((shares,)),
            dma((groups,)),
            dma((groups,)),
        ],
        compiler_params=pltpu.CompilerParams(
            collective_id=0, has_side_effects=True, vmem_limit_bytes=20 * 1024 * 1024
        ),
    )(partial, lse, out_weight)


def solution(mesh):
    in_specs = (
        P(None, "kvh", None),
        P("seq", "kvh", None, None),
        P("seq", "kvh", None, None),
        P("seq", "kvh", None, None),
        P("seq", "kvh", None, None),
        P(None, "kvh", None),
        P("seq"),
        P("kvh", "seq"),
    )
    return jax.shard_map(
        functools.partial(on_device, mesh.shape["seq"], mesh.shape["kvh"]),
        mesh=mesh, in_specs=in_specs, out_specs=P("kvh", "seq"), check_vma=False,
    )
```

```python
import functools
import math

import jax
import jax.numpy as jnp
from jax import lax
from jax.experimental import pallas as pl
from jax.experimental.pallas import tpu as pltpu
from jax.sharding import PartitionSpec as P

FLOOR_SCORE = -1e30
LANES = 128
UNROLL = 16
PIECES = 4
MESH = pl.DeviceIdType.MESH


def contract_last(a, b):
    return lax.dot_general(a, b, (((1,), (1,)), ((), ())), preferred_element_type=jnp.float32)


def matmul(a, b):
    return jnp.dot(a, b, preferred_element_type=jnp.float32)


def attend_kernel(
    counts_hbm, ids_hbm, q_hbm, rk_hbm, rv_hbm, keys_ref, values_ref, o_ref, lse_ref,
    counts_ref, ids_ref, q_ref, rk_mem, rv_mem,
    k_mem, v_mem, slots_v, slots_s, qh, sums, sc, top, low, acc, k_sem, v_sem, slot_sem, in_sem,
):
    tokens, heads, width = q_ref.shape
    kv_heads, blocks, span, _ = k_mem.shape
    group = heads // kv_heads
    reps = blocks * rk_mem.shape[2]
    chosen = ids_ref.shape[1]
    lanes = slots_v.shape[1]
    inv_root = 1.0 / math.sqrt(width)
    me = lax.axis_index("seq")

    part = blocks // PIECES

    def copy_of(k, i, source, target, sem):
        rows = pl.ds(i * part, part)
        return pltpu.make_async_copy(source.at[rows, k], target.at[k, rows], sem.at[k, i])

    ids_copy = pltpu.make_async_copy(ids_hbm, ids_ref, in_sem.at[0])
    counts_copy = pltpu.make_async_copy(counts_hbm, counts_ref, in_sem.at[1])
    q_copy = pltpu.make_async_copy(q_hbm, q_ref, in_sem.at[2])
    rk_copies = [
        pltpu.make_async_copy(rk_hbm.at[:, k], rk_mem.at[k], in_sem.at[3 + k])
        for k in range(kv_heads)
    ]
    rv_copies = [
        pltpu.make_async_copy(rv_hbm.at[:, k], rv_mem.at[k], in_sem.at[3 + kv_heads + k])
        for k in range(kv_heads)
    ]
    for copy in [ids_copy, counts_copy, q_copy] + rk_copies + rv_copies:
        copy.start()
    for k in range(kv_heads):
        for i in range(PIECES):
            copy_of(k, i, keys_ref, k_mem, k_sem).start()
        for i in range(PIECES):
            copy_of(k, i, values_ref, v_mem, v_sem).start()

    token_of = lax.broadcasted_iota(jnp.int32, (tokens, chosen), 0)
    slot_of = lax.broadcasted_iota(jnp.int32, (tokens, lanes), 1)
    before_slot = (
        lax.broadcasted_iota(jnp.int32, (chosen, chosen), 0)
        < lax.broadcasted_iota(jnp.int32, (chosen, chosen), 1)
    ).astype(jnp.bfloat16)
    before_token = (
        lax.broadcasted_iota(jnp.int32, (tokens, tokens), 1)
        < lax.broadcasted_iota(jnp.int32, (tokens, tokens), 0)
    ).astype(jnp.bfloat16)
    same_token = (
        lax.broadcasted_iota(jnp.int32, (tokens, tokens), 1)
        == lax.broadcasted_iota(jnp.int32, (tokens, tokens), 0)
    ).astype(jnp.bfloat16)
    every_slot = jnp.ones((chosen, chosen), jnp.bfloat16)
    slots_v[...] = jnp.zeros_like(slots_v)
    ids_copy.wait()
    for k in range(kv_heads):
        ids = ids_ref[k] - me * blocks
        ids = jnp.where((ids >= 0) & (ids < blocks), ids + 1, 0).astype(jnp.float32)
        place = contract_last(same_token, ids.astype(jnp.bfloat16)).astype(jnp.int32)
        here = place > 0
        mark = jnp.where(here, 1.0, 0.0).astype(jnp.bfloat16)
        of_token = matmul(mark, every_slot)
        rank = matmul(mark, before_slot) + matmul(before_token, of_token.astype(jnp.bfloat16))
        rank = jnp.where(here, rank.astype(jnp.int32), -1)
        code = token_of * blocks + place
        found = jnp.zeros((tokens, lanes), jnp.int32)
        for s in range(chosen):
            found = found + jnp.where(rank[:, s : s + 1] == slot_of, code[:, s : s + 1], 0)
        slots_v[k : k + 1, :] = jnp.sum(found, axis=0, keepdims=True)
        total = jnp.sum(of_token[:, 0:1], axis=0, keepdims=True).astype(jnp.int32)
        slots_v[kv_heads + k : kv_heads + k + 1, :] = jnp.broadcast_to(total, (1, lanes))
    slot_copy = pltpu.make_async_copy(slots_v, slots_s, slot_sem)
    slot_copy.start()

    for copy in [q_copy] + rk_copies:
        copy.wait()
    for k in range(kv_heads):
        mine = q_ref[...].astype(jnp.float32)[:, k * group : (k + 1) * group, :]
        qh[k] = mine.reshape(tokens * group, width).astype(jnp.bfloat16)
        scores = contract_last(qh[k], rk_mem[k].reshape(reps, width)) * inv_root
        sums[k] = scores
        most = scores[:, :LANES]
        for c in range(LANES, reps, LANES):
            most = jnp.maximum(most, scores[:, c : c + LANES])
        top[k] = most.reshape(tokens, group, LANES)

    for copy in [slot_copy, counts_copy] + rv_copies:
        copy.wait()
    lane = lax.broadcasted_iota(jnp.int32, (group, span), 1)

    def slot(k, j):
        code = slots_s[k, j]
        at = jnp.maximum(code - 1, 0)
        token = lax.div(at, blocks)
        return code, token, at - token * blocks

    for k in range(kv_heads):
        rounds = lax.div(slots_s[kv_heads + k, 0] + (UNROLL - 1), UNROLL)

        for i in range(PIECES):
            copy_of(k, i, keys_ref, k_mem, k_sem).wait()

        def score_round(i, carry, k=k):
            places, found = [], []
            for u in range(UNROLL):
                j = i * UNROLL + u
                code, token, block = slot(k, j)
                count = jnp.where(code > 0, counts_ref[block], 0)
                s = contract_last(q_ref[token], k_mem[k, block])
                s = s[k * group : (k + 1) * group] * inv_root
                s = jnp.where(lane < count, s, FLOOR_SCORE)
                sc[j] = s
                places.append(token)
                found.append(s)
            for token, s in zip(places, found):
                top[k, token] = jnp.maximum(top[k, token], s)
            return carry

        lax.fori_loop(0, rounds, score_round, 0)

        most = jnp.max(top[k], axis=2, keepdims=True)
        top[k] = jnp.broadcast_to(most, (tokens, group, LANES))
        weights = jnp.exp(sums[k] - most.reshape(tokens * group, 1))
        some = weights[:, :LANES]
        for c in range(LANES, reps, LANES):
            some = some + weights[:, c : c + LANES]
        low[k] = some.reshape(tokens, group, LANES)
        acc[k] = matmul(weights.astype(jnp.bfloat16), rv_mem[k].reshape(reps, width)).reshape(tokens, group, width)

        for i in range(PIECES):
            copy_of(k, i, values_ref, v_mem, v_sem).wait()

        def weight_round(i, carry, k=k):
            places, found, parts = [], [], []
            for u in range(UNROLL):
                j = i * UNROLL + u
                _, token, block = slot(k, j)
                p = jnp.exp(sc[j] - top[k, token])
                places.append(token)
                found.append(p)
                parts.append(matmul(p.astype(jnp.bfloat16), v_mem[k, block]))
            for token, p, o in zip(places, found, parts):
                low[k, token] = low[k, token] + p
                acc[k, token] = acc[k, token] + o
            return carry

        lax.fori_loop(0, rounds, weight_round, 0)

        weight_sum = jnp.sum(low[k], axis=2, keepdims=True)
        low[k] = top[k] + jnp.log(jnp.broadcast_to(weight_sum, (tokens, group, LANES)))
        acc[k] = acc[k] / weight_sum

    shares, rows, _ = o_ref.shape
    run = min(rows, tokens)
    diagonal = lax.broadcasted_iota(jnp.int32, (run, LANES), 0)
    column = lax.broadcasted_iota(jnp.int32, (run, LANES), 1)
    for share in range(shares):
        line = jnp.zeros((1, LANES), jnp.float32)
        for at in range(0, rows, run):
            head, token = divmod(share * rows + at, tokens)
            k, g = divmod(head, group)
            o_ref[share, at : at + run, :] = acc[k, token : token + run, g, :].astype(jnp.bfloat16)
            lse = low[k, token : token + run, g, :]
            line += jnp.sum(
                jnp.where(diagonal + at == column, lse, 0.0), axis=0, keepdims=True
            )
        lse_ref[share] = jnp.broadcast_to(line, lse_ref.shape[1:])


def finish_kernel(
    shares, groups, o_ref, lse_ref, w_ref, out_ref,
    w_mem, o_in, lse_in, attended, total, part_out, part_in,
    w_sem, o_send, o_recv, lse_send, lse_recv, a_send, a_recv, p_send, p_recv,
):
    me, mine = lax.axis_index("seq"), lax.axis_index("kvh")
    _, rows, width = o_ref.shape
    tokens, columns = total.shape

    def w_copy(i):
        depth = w_ref.shape[0] // shares
        return pltpu.make_async_copy(
            w_ref.at[pl.ds(i * depth, depth)], w_mem.at[pl.ds(i * depth, depth)], w_sem.at[i]
        )

    for i in range(shares):
        w_copy(i).start()

    barrier = pltpu.get_barrier_semaphore()
    for d in range(1, shares):
        pl.semaphore_signal(
            barrier, inc=1, device_id={"seq": lax.rem(me + d, shares)}, device_id_type=MESH
        )
    for d in range(1, groups):
        pl.semaphore_signal(
            barrier, inc=1, device_id={"kvh": lax.rem(mine + d, groups)}, device_id_type=MESH
        )
    pl.semaphore_wait(barrier, shares - 1 + groups - 1)

    def send(source, target, sent, got, axis, peer):
        copy = pltpu.make_async_remote_copy(
            src_ref=source, dst_ref=target, send_sem=sent, recv_sem=got,
            device_id={axis: peer}, device_id_type=MESH,
        )
        copy.start()
        return copy

    spread = []
    for d in range(1, shares):
        peer = lax.rem(me + d, shares)
        spread.append(send(
            lse_ref.at[peer], lse_in.at[me], lse_send.at[d], lse_recv.at[d], "seq", peer))
        spread.append(send(o_ref.at[peer], o_in.at[me], o_send.at[d], o_recv.at[d], "seq", peer))
    lse_in[me] = lse_ref[me]
    o_in[me] = o_ref[me]
    for copy in spread:
        copy.wait_recv()

    lse = [lse_in[i][0:1] for i in range(shares)]
    highest = functools.reduce(jnp.maximum, lse)
    factors = [jnp.exp(one - highest) for one in lse]
    inverse = 1.0 / functools.reduce(jnp.add, factors)
    on_diagonal = lax.broadcasted_iota(jnp.int32, (rows, LANES), 0) == lax.broadcasted_iota(
        jnp.int32, (rows, LANES), 1
    )
    joined = jnp.zeros((rows, width), jnp.float32)
    for i in range(shares):
        factor = jnp.where(on_diagonal, factors[i] * inverse, 0.0)
        joined += jnp.sum(factor, axis=1, keepdims=True) * o_in[i].astype(jnp.float32)
    attended[me] = joined.astype(jnp.bfloat16)

    gathered = []
    for d in range(1, shares):
        peer = lax.rem(me + d, shares)
        gathered.append(send(
            attended.at[me], attended.at[me], a_send.at[d], a_recv.at[d], "seq", peer))

    for i in range(shares):
        w_copy(i).wait()
    if rows % tokens == 0:
        depth = rows // tokens * width
        for d in range(shares):
            if d:
                gathered[d - 1].wait_recv()
            owner = lax.rem(me - d + shares, shares)
            block = attended[owner]
            left = jnp.concatenate(
                [block[at : at + tokens] for at in range(0, rows, tokens)], axis=1
            )
            right = w_mem[pl.ds(pl.multiple_of(owner * depth, depth), depth), :]
            term = matmul(left, right)
            total[...] = term if d == 0 else total[...] + term
    else:
        for copy in gathered:
            copy.wait_recv()
        pieces = tokens // rows
        for head in range(shares // pieces):
            left = jnp.concatenate([attended[head * pieces + p] for p in range(pieces)], axis=0)
            term = matmul(left, w_mem[head * width : (head + 1) * width, :])
            total[...] = term if head == 0 else total[...] + term

    here = tokens // groups
    part_out[...] = total[...].astype(jnp.bfloat16).reshape(part_out.shape)
    parts = []
    for d in range(1, groups):
        peer = lax.rem(mine + d, groups)
        parts.append(send(
            part_out.at[peer], part_in.at[mine], p_send.at[d], p_recv.at[d], "kvh", peer))
    result = total[pl.ds(pl.multiple_of(mine * here, here), here), :]
    for d in range(1, groups):
        parts[d - 1].wait_recv()
        result = result + part_in[lax.rem(mine - d + groups, groups)].astype(jnp.float32)
    out_ref[...] = result.astype(out_ref.dtype)
    for copy in spread + gathered + parts:
        copy.wait_send()


def on_device(
    shares, groups, queries, keys, values, rep_keys, rep_values, block_ids, block_counts, out_weight
):
    tokens, heads, width = queries.shape
    blocks, kv_heads, span, _ = keys.shape
    group = heads // kv_heads
    reps = blocks * rep_keys.shape[2]
    rows = heads * tokens // shares
    columns = out_weight.shape[1]
    capacity = -(-3 * tokens // UNROLL) * UNROLL
    lanes = -(-capacity // LANES) * LANES
    vmem = pl.BlockSpec(memory_space=pltpu.VMEM)
    by_slot = jnp.transpose(block_ids, (1, 2, 0))
    hbm = pl.BlockSpec(memory_space=pltpu.HBM)
    dma = pltpu.SemaphoreType.DMA

    partial, lse = pl.pallas_call(
        attend_kernel,
        out_shape=(
            jax.ShapeDtypeStruct((shares, rows, width), jnp.bfloat16),
            jax.ShapeDtypeStruct((shares, 8, LANES), jnp.float32),
        ),
        in_specs=[hbm] * 7,
        out_specs=(vmem, vmem),
        scratch_shapes=[
            pltpu.SMEM(block_counts.shape, jnp.int32),
            pltpu.VMEM(by_slot.shape, jnp.int32),
            pltpu.VMEM(queries.shape, jnp.bfloat16),
            pltpu.VMEM((kv_heads, blocks) + rep_keys.shape[2:], jnp.bfloat16),
            pltpu.VMEM((kv_heads, blocks) + rep_keys.shape[2:], jnp.bfloat16),
            pltpu.VMEM((kv_heads, blocks, span, width), jnp.bfloat16),
            pltpu.VMEM((kv_heads, blocks, span, width), jnp.bfloat16),
            pltpu.VMEM((8, lanes), jnp.int32),
            pltpu.SMEM((8, lanes), jnp.int32),
            pltpu.VMEM((kv_heads, tokens * group, width), jnp.bfloat16),
            pltpu.VMEM((kv_heads, tokens * group, reps), jnp.float32),
            pltpu.VMEM((capacity, group, span), jnp.float32),
            pltpu.VMEM((kv_heads, tokens, group, LANES), jnp.float32),
            pltpu.VMEM((kv_heads, tokens, group, LANES), jnp.float32),
            pltpu.VMEM((kv_heads, tokens, group, width), jnp.float32),
            dma((kv_heads, PIECES)),
            dma((kv_heads, PIECES)),
            dma,
            dma((3 + 2 * kv_heads,)),
        ],
        compiler_params=pltpu.CompilerParams(vmem_limit_bytes=67043328),
    )(block_counts, by_slot, queries, rep_keys, rep_values, keys, values)

    return pl.pallas_call(
        functools.partial(finish_kernel, shares, groups),
        out_shape=jax.ShapeDtypeStruct((tokens // groups, columns), jnp.bfloat16),
        in_specs=[vmem, vmem, hbm],
        out_specs=vmem,
        scratch_shapes=[
            pltpu.VMEM(out_weight.shape, jnp.bfloat16),
            pltpu.VMEM((shares, rows, width), jnp.bfloat16),
            pltpu.VMEM((shares, 8, LANES), jnp.float32),
            pltpu.VMEM((shares, rows, width), jnp.bfloat16),
            pltpu.VMEM((tokens, columns), jnp.float32),
            pltpu.VMEM((groups, tokens // groups, columns), jnp.bfloat16),
            pltpu.VMEM((groups, tokens // groups, columns), jnp.bfloat16),
            dma((shares,)),
            dma((shares,)),
            dma((shares,)),
            dma((shares,)),
            dma((shares,)),
            dma((shares,)),
            dma((shares,)),
            dma((groups,)),
            dma((groups,)),
        ],
        compiler_params=pltpu.CompilerParams(
            collective_id=0, has_side_effects=True, vmem_limit_bytes=60 * 1024 * 1024
        ),
    )(partial, lse, out_weight)


def solution(mesh):
    in_specs = (
        P(None, "kvh", None),
        P("seq", "kvh", None, None),
        P("seq", "kvh", None, None),
        P("seq", "kvh", None, None),
        P("seq", "kvh", None, None),
        P(None, "kvh", None),
        P("seq"),
        P("kvh", "seq"),
    )
    return jax.shard_map(
        functools.partial(on_device, mesh.shape["seq"], mesh.shape["kvh"]),
        mesh=mesh, in_specs=in_specs, out_specs=P("kvh", "seq"), check_vma=False,
    )
```

```python
import functools
import math

import jax
import jax.numpy as jnp
from jax import lax
from jax.experimental import pallas as pl
from jax.experimental.pallas import tpu as pltpu
from jax.sharding import PartitionSpec as P

FLOOR_SCORE = -1e30
LANES = 128
UNROLL = 16
PIECES = 4
MESH = pl.DeviceIdType.MESH


def contract_last(a, b):
    return lax.dot_general(a, b, (((1,), (1,)), ((), ())), preferred_element_type=jnp.float32)


def matmul(a, b):
    return jnp.dot(a, b, preferred_element_type=jnp.float32)


def attend_kernel(
    counts_hbm, ids_hbm, q_hbm, rk_hbm, rv_hbm, keys_ref, values_ref, o_ref, stat_ref,
    counts_ref, ids_ref, q_ref, rk_mem, rv_mem,
    k_mem, v_mem, slots_v, slots_s, qh, sums, sc, top, low, acc, k_sem, v_sem, slot_sem, in_sem,
):
    tokens, heads, width = q_ref.shape
    kv_heads, blocks, span, _ = k_mem.shape
    group = heads // kv_heads
    reps = blocks * rk_mem.shape[2]
    chosen = ids_ref.shape[1]
    lanes = slots_v.shape[1]
    scale = math.log2(math.e) / math.sqrt(width)
    me = lax.axis_index("seq")

    part = blocks // PIECES

    def copy_of(k, i, source, target, sem):
        rows = pl.ds(i * part, part)
        return pltpu.make_async_copy(source.at[rows, k], target.at[k, rows], sem.at[k, i])

    ids_copy = pltpu.make_async_copy(ids_hbm, ids_ref, in_sem.at[0])
    counts_copy = pltpu.make_async_copy(counts_hbm, counts_ref, in_sem.at[1])
    q_copy = pltpu.make_async_copy(q_hbm, q_ref, in_sem.at[2])
    rk_copies = [
        pltpu.make_async_copy(rk_hbm.at[:, k], rk_mem.at[k], in_sem.at[3 + k])
        for k in range(kv_heads)
    ]
    rv_copies = [
        pltpu.make_async_copy(rv_hbm.at[:, k], rv_mem.at[k], in_sem.at[3 + kv_heads + k])
        for k in range(kv_heads)
    ]
    for copy in [ids_copy, counts_copy, q_copy] + rk_copies + rv_copies:
        copy.start()
    for k in range(kv_heads):
        for i in range(PIECES):
            copy_of(k, i, keys_ref, k_mem, k_sem).start()
        for i in range(PIECES):
            copy_of(k, i, values_ref, v_mem, v_sem).start()

    token_of = lax.broadcasted_iota(jnp.int32, (tokens, chosen), 0)
    slot_of = lax.broadcasted_iota(jnp.int32, (tokens, lanes), 1)
    before_slot = (
        lax.broadcasted_iota(jnp.int32, (chosen, chosen), 0)
        < lax.broadcasted_iota(jnp.int32, (chosen, chosen), 1)
    ).astype(jnp.bfloat16)
    before_token = (
        lax.broadcasted_iota(jnp.int32, (tokens, tokens), 1)
        < lax.broadcasted_iota(jnp.int32, (tokens, tokens), 0)
    ).astype(jnp.bfloat16)
    same_token = (
        lax.broadcasted_iota(jnp.int32, (tokens, tokens), 1)
        == lax.broadcasted_iota(jnp.int32, (tokens, tokens), 0)
    ).astype(jnp.bfloat16)
    every_slot = jnp.ones((chosen, chosen), jnp.bfloat16)
    slots_v[...] = jnp.zeros_like(slots_v)
    ids_copy.wait()
    for k in range(kv_heads):
        ids = ids_ref[k] - me * blocks
        ids = jnp.where((ids >= 0) & (ids < blocks), ids + 1, 0).astype(jnp.float32)
        place = contract_last(same_token, ids.astype(jnp.bfloat16)).astype(jnp.int32)
        here = place > 0
        mark = jnp.where(here, 1.0, 0.0).astype(jnp.bfloat16)
        of_token = matmul(mark, every_slot)
        rank = matmul(mark, before_slot) + matmul(before_token, of_token.astype(jnp.bfloat16))
        rank = jnp.where(here, rank.astype(jnp.int32), -1)
        code = token_of * blocks + place
        found = jnp.zeros((tokens, lanes), jnp.int32)
        for s in range(chosen):
            found = found + jnp.where(rank[:, s : s + 1] == slot_of, code[:, s : s + 1], 0)
        slots_v[k : k + 1, :] = jnp.sum(found, axis=0, keepdims=True)
        total = jnp.sum(of_token[:, 0:1], axis=0, keepdims=True).astype(jnp.int32)
        slots_v[kv_heads + k : kv_heads + k + 1, :] = jnp.broadcast_to(total, (1, lanes))
    slot_copy = pltpu.make_async_copy(slots_v, slots_s, slot_sem)
    slot_copy.start()

    for copy in [q_copy] + rk_copies:
        copy.wait()
    for k in range(kv_heads):
        mine = q_ref[...].astype(jnp.float32)[:, k * group : (k + 1) * group, :]
        qh[k] = mine.reshape(tokens * group, width).astype(jnp.bfloat16)
        scores = contract_last(qh[k], rk_mem[k].reshape(reps, width))
        sums[k] = scores
        most = scores[:, :LANES]
        for c in range(LANES, reps, LANES):
            most = jnp.maximum(most, scores[:, c : c + LANES])
        top[k] = most.reshape(tokens, group, LANES)

    for copy in [slot_copy, counts_copy] + rv_copies:
        copy.wait()
    lane = lax.broadcasted_iota(jnp.int32, (group, span), 1)

    def slot(k, j):
        code = slots_s[k, j]
        at = jnp.maximum(code - 1, 0)
        token = lax.div(at, blocks)
        return code, token, at - token * blocks

    for k in range(kv_heads):
        rounds = lax.div(slots_s[kv_heads + k, 0] + (UNROLL - 1), UNROLL)

        for i in range(PIECES):
            copy_of(k, i, keys_ref, k_mem, k_sem).wait()

        def score_round(i, carry, k=k):
            places, found = [], []
            for u in range(UNROLL):
                j = i * UNROLL + u
                code, token, block = slot(k, j)
                count = jnp.where(code > 0, counts_ref[block], 0)
                s = contract_last(q_ref[token], k_mem[k, block])
                s = s[k * group : (k + 1) * group]
                s = jnp.where(lane < count, s, FLOOR_SCORE)
                sc[j] = s
                places.append(token)
                found.append(s)
            for token, s in zip(places, found):
                top[k, token] = jnp.maximum(top[k, token], s)
            return carry

        lax.fori_loop(0, rounds, score_round, 0)

        most = jnp.max(top[k], axis=2, keepdims=True)
        top[k] = jnp.broadcast_to(most, (tokens, group, LANES))
        weights = jnp.exp2((sums[k] - most.reshape(tokens * group, 1)) * scale)
        some = weights[:, :LANES]
        for c in range(LANES, reps, LANES):
            some = some + weights[:, c : c + LANES]
        low[k] = some.reshape(tokens, group, LANES)
        acc[k] = matmul(weights.astype(jnp.bfloat16), rv_mem[k].reshape(reps, width)).reshape(tokens, group, width)

        for i in range(PIECES):
            copy_of(k, i, values_ref, v_mem, v_sem).wait()

        def weight_round(i, carry, k=k):
            places, found, parts = [], [], []
            for u in range(UNROLL):
                j = i * UNROLL + u
                _, token, block = slot(k, j)
                p = jnp.exp2((sc[j] - top[k, token]) * scale)
                places.append(token)
                found.append(p)
                parts.append(matmul(p.astype(jnp.bfloat16), v_mem[k, block]))
            for token, p, o in zip(places, found, parts):
                low[k, token] = low[k, token] + p
                acc[k, token] = acc[k, token] + o
            return carry

        lax.fori_loop(0, rounds, weight_round, 0)

    shares, rows, _ = o_ref.shape
    run = min(rows, tokens)
    diagonal = lax.broadcasted_iota(jnp.int32, (run, LANES), 0)
    column = lax.broadcasted_iota(jnp.int32, (run, LANES), 1)
    top_rows, low_rows, acc_rows = (
        one.reshape(kv_heads * tokens * group, LANES) for one in (top, low, acc)
    )
    ones = jnp.ones((8, LANES), jnp.bfloat16)
    first = lax.broadcasted_iota(jnp.int32, (8, LANES), 0) == 0
    for share in range(shares):
        line = jnp.zeros((1, LANES), jnp.float32)
        parts = []
        for at in range(0, rows, run):
            head, token = divmod(share * rows + at, tokens)
            k, g = divmod(head, group)
            picked = pl.ds((k * tokens + token) * group + g, run, stride=group)
            o_ref[share, at : at + run, :] = acc_rows[picked, :].astype(jnp.bfloat16)
            most = top_rows[picked, :] * scale
            line += jnp.sum(
                jnp.where(diagonal + at == column, most, 0.0), axis=0, keepdims=True
            )
            parts.append(low_rows[picked, :])
        if rows < LANES:
            parts.append(jnp.zeros((LANES - rows, LANES), jnp.float32))
        part = jnp.concatenate(parts, axis=0)
        coarse = part.astype(jnp.bfloat16)
        fine = (part - coarse.astype(jnp.float32)).astype(jnp.bfloat16)
        weight_sum = contract_last(ones, coarse) + contract_last(ones, fine)
        stat_ref[share] = jnp.where(first, line, weight_sum)


def finish_kernel(
    shares, groups, o_ref, stat_ref, w_ref, out_ref,
    w_mem, o_in, stat_in, attended, total, part_out, part_in,
    w_sem, o_send, o_recv, stat_send, stat_recv, a_send, a_recv, p_send, p_recv,
):
    me, mine = lax.axis_index("seq"), lax.axis_index("kvh")
    _, rows, width = o_ref.shape
    tokens, columns = total.shape

    def w_copy(i):
        depth = w_ref.shape[0] // shares
        return pltpu.make_async_copy(
            w_ref.at[pl.ds(i * depth, depth)], w_mem.at[pl.ds(i * depth, depth)], w_sem.at[i]
        )

    for i in range(shares):
        w_copy(i).start()

    barrier = pltpu.get_barrier_semaphore()
    for d in range(1, shares):
        pl.semaphore_signal(
            barrier, inc=1, device_id={"seq": lax.rem(me + d, shares)}, device_id_type=MESH
        )
    for d in range(1, groups):
        pl.semaphore_signal(
            barrier, inc=1, device_id={"kvh": lax.rem(mine + d, groups)}, device_id_type=MESH
        )
    pl.semaphore_wait(barrier, shares - 1 + groups - 1)

    def send(source, target, sent, got, axis, peer):
        copy = pltpu.make_async_remote_copy(
            src_ref=source, dst_ref=target, send_sem=sent, recv_sem=got,
            device_id={axis: peer}, device_id_type=MESH,
        )
        copy.start()
        return copy

    spread = []
    for d in range(1, shares):
        peer = lax.rem(me + d, shares)
        spread.append(send(
            stat_ref.at[peer], stat_in.at[me], stat_send.at[d], stat_recv.at[d], "seq", peer))
        spread.append(send(o_ref.at[peer], o_in.at[me], o_send.at[d], o_recv.at[d], "seq", peer))
    stat_in[me] = stat_ref[me]
    o_in[me] = o_ref[me]
    for copy in spread:
        copy.wait_recv()

    tops = [stat_in[i][0:1] for i in range(shares)]
    highest = functools.reduce(jnp.maximum, tops)
    factors = [jnp.exp2(one - highest) for one in tops]
    inverse = 1.0 / functools.reduce(
        jnp.add, [factors[i] * stat_in[i][1:2] for i in range(shares)]
    )
    on_diagonal = lax.broadcasted_iota(jnp.int32, (rows, LANES), 0) == lax.broadcasted_iota(
        jnp.int32, (rows, LANES), 1
    )
    joined = jnp.zeros((rows, width), jnp.float32)
    for i in range(shares):
        factor = jnp.where(on_diagonal, factors[i] * inverse, 0.0)
        joined += jnp.sum(factor, axis=1, keepdims=True) * o_in[i].astype(jnp.float32)
    attended[me] = joined.astype(jnp.bfloat16)

    gathered = []
    for d in range(1, shares):
        peer = lax.rem(me + d, shares)
        gathered.append(send(
            attended.at[me], attended.at[me], a_send.at[d], a_recv.at[d], "seq", peer))

    for i in range(shares):
        w_copy(i).wait()
    if rows % tokens == 0:
        depth = rows // tokens * width
        for d in range(shares):
            if d:
                gathered[d - 1].wait_recv()
            owner = lax.rem(me - d + shares, shares)
            block = attended[owner]
            left = jnp.concatenate(
                [block[at : at + tokens] for at in range(0, rows, tokens)], axis=1
            )
            right = w_mem[pl.ds(pl.multiple_of(owner * depth, depth), depth), :]
            term = matmul(left, right)
            total[...] = term if d == 0 else total[...] + term
    else:
        for copy in gathered:
            copy.wait_recv()
        pieces = tokens // rows
        for head in range(shares // pieces):
            left = jnp.concatenate([attended[head * pieces + p] for p in range(pieces)], axis=0)
            term = matmul(left, w_mem[head * width : (head + 1) * width, :])
            total[...] = term if head == 0 else total[...] + term

    here = tokens // groups
    part_out[...] = total[...].astype(jnp.bfloat16).reshape(part_out.shape)
    parts = []
    for d in range(1, groups):
        peer = lax.rem(mine + d, groups)
        parts.append(send(
            part_out.at[peer], part_in.at[mine], p_send.at[d], p_recv.at[d], "kvh", peer))
    result = total[pl.ds(pl.multiple_of(mine * here, here), here), :]
    for d in range(1, groups):
        parts[d - 1].wait_recv()
        result = result + part_in[lax.rem(mine - d + groups, groups)].astype(jnp.float32)
    out_ref[...] = result.astype(out_ref.dtype)
    for copy in spread + gathered + parts:
        copy.wait_send()


def on_device(
    shares, groups, queries, keys, values, rep_keys, rep_values, block_ids, block_counts, out_weight
):
    tokens, heads, width = queries.shape
    blocks, kv_heads, span, _ = keys.shape
    group = heads // kv_heads
    reps = blocks * rep_keys.shape[2]
    rows = heads * tokens // shares
    columns = out_weight.shape[1]
    capacity = -(-3 * tokens // UNROLL) * UNROLL
    lanes = -(-capacity // LANES) * LANES
    vmem = pl.BlockSpec(memory_space=pltpu.VMEM)
    by_slot = jnp.transpose(block_ids, (1, 2, 0))
    queries, keys, values, rep_keys, rep_values, block_counts, by_slot, out_weight = (
        pltpu.with_memory_space_constraint(one, pltpu.HBM)
        for one in (
            queries, keys, values, rep_keys, rep_values, block_counts, by_slot, out_weight
        )
    )
    hbm = pl.BlockSpec(memory_space=pltpu.HBM)
    dma = pltpu.SemaphoreType.DMA

    partial, stats = pl.pallas_call(
        attend_kernel,
        out_shape=(
            jax.ShapeDtypeStruct((shares, rows, width), jnp.bfloat16),
            jax.ShapeDtypeStruct((shares, 8, LANES), jnp.float32),
        ),
        in_specs=[hbm] * 7,
        out_specs=(vmem, vmem),
        scratch_shapes=[
            pltpu.SMEM(block_counts.shape, jnp.int32),
            pltpu.VMEM(by_slot.shape, jnp.int32),
            pltpu.VMEM(queries.shape, jnp.bfloat16),
            pltpu.VMEM((kv_heads, blocks) + rep_keys.shape[2:], jnp.bfloat16),
            pltpu.VMEM((kv_heads, blocks) + rep_keys.shape[2:], jnp.bfloat16),
            pltpu.VMEM((kv_heads, blocks, span, width), jnp.bfloat16),
            pltpu.VMEM((kv_heads, blocks, span, width), jnp.bfloat16),
            pltpu.VMEM((8, lanes), jnp.int32),
            pltpu.SMEM((8, lanes), jnp.int32),
            pltpu.VMEM((kv_heads, tokens * group, width), jnp.bfloat16),
            pltpu.VMEM((kv_heads, tokens * group, reps), jnp.float32),
            pltpu.VMEM((capacity, group, span), jnp.float32),
            pltpu.VMEM((kv_heads, tokens, group, LANES), jnp.float32),
            pltpu.VMEM((kv_heads, tokens, group, LANES), jnp.float32),
            pltpu.VMEM((kv_heads, tokens, group, width), jnp.float32),
            dma((kv_heads, PIECES)),
            dma((kv_heads, PIECES)),
            dma,
            dma((3 + 2 * kv_heads,)),
        ],
        compiler_params=pltpu.CompilerParams(vmem_limit_bytes=32 * 1024 * 1024),
    )(block_counts, by_slot, queries, rep_keys, rep_values, keys, values)

    return pl.pallas_call(
        functools.partial(finish_kernel, shares, groups),
        out_shape=jax.ShapeDtypeStruct((tokens // groups, columns), jnp.bfloat16),
        in_specs=[vmem, vmem, hbm],
        out_specs=vmem,
        scratch_shapes=[
            pltpu.VMEM(out_weight.shape, jnp.bfloat16),
            pltpu.VMEM((shares, rows, width), jnp.bfloat16),
            pltpu.VMEM((shares, 8, LANES), jnp.float32),
            pltpu.VMEM((shares, rows, width), jnp.bfloat16),
            pltpu.VMEM((tokens, columns), jnp.float32),
            pltpu.VMEM((groups, tokens // groups, columns), jnp.bfloat16),
            pltpu.VMEM((groups, tokens // groups, columns), jnp.bfloat16),
            dma((shares,)),
            dma((shares,)),
            dma((shares,)),
            dma((shares,)),
            dma((shares,)),
            dma((shares,)),
            dma((shares,)),
            dma((groups,)),
            dma((groups,)),
        ],
        compiler_params=pltpu.CompilerParams(
            collective_id=0, has_side_effects=True, vmem_limit_bytes=20 * 1024 * 1024
        ),
    )(partial, stats, out_weight)


def solution(mesh):
    in_specs = (
        P(None, "kvh", None),
        P("seq", "kvh", None, None),
        P("seq", "kvh", None, None),
        P("seq", "kvh", None, None),
        P("seq", "kvh", None, None),
        P(None, "kvh", None),
        P("seq"),
        P("kvh", "seq"),
    )
    return jax.shard_map(
        functools.partial(on_device, mesh.shape["seq"], mesh.shape["kvh"]),
        mesh=mesh, in_specs=in_specs, out_specs=P("kvh", "seq"), check_vma=False,
    )
```
